32 devices in a mesh: member: 2 (over y), blk: 16 (over z, x, core).
Axes of the slice: x: 2, y: 2, z: 4, core: 2. Of those that a mesh axis runs over, the one named last changes fastest.
Arguments:
- heat_anomaly: float32 [8, 1536, 512], P('member', 'blk'), parts along dimension 0, may hold values from -6 to 6
- saltiness_anomaly: float32 [8, 1536, 512], P('member', 'blk'), parts along dimension 0, may hold values from -6 to 6
- first_axis_flow: float32 [8, 1536, 512], P('member', 'blk'), parts along dimension 0, may hold values from -4 to 4
- second_axis_flow: float32 [8, 1536, 512], P('member', 'blk'), parts along dimension 0, may hold values from -4 to 4
- layer_spacing: float32 [4], replicated, may hold values from 0.5 to 4
- diagonal_shift: float32 [1536, 512], P('blk'), may hold values from 0.02 to 0.2
- water_tile_flags: int32 [16, 8], P('blk'), may hold values 0 or 1
Outputs:
- new_temperature: bfloat16 [8, 1536, 512], P('member', 'blk'), parts along dimension 0
- new_salinity: bfloat16 [8, 1536, 512], P('member', 'blk'), parts along dimension 0
- new_u: bfloat16 [8, 1536, 512], P('member', 'blk'), parts along dimension 0
- new_v: bfloat16 [8, 1536, 512], P('member', 'blk'), parts along dimension 0
- height: float32 [3072, 512], P(('member', 'blk')), parts along dimension 0
- residual: float32 [3072, 512], P(('member', 'blk')), parts along dimension 0
The draws below stay inside these ranges and needn't reach their ends.
There are 2 independent parts, one for each index of `member`. The reference program is written for one: setup_inputs(seed, part) draws one part's arguments, and reference() takes and returns one part's arrays. A program takes and returns all parts, laid end to end along the dimension named above; an argument that names none is the same for every part. Nothing has to cross between parts.
Inputs may be any that keep to these rules, and one draw needn't show every extreme that they name: `water_tile_flags`: 1 marks an ocean block, 0 a land block.
All inputs are finite; a program needn't handle non-finite values.
Results may differ from the reference program's by a relative error of at most 0.001.
Values sent between devices are 32-bit elements; how exact they have to be, the bound alone decides.
A program may use at most 128 MiB of HBM per device.

```python
import math
import jax
import jax.numpy as jnp
import numpy as np
from jax import lax

BX = 96
BY = 64
HOME = 8
LAYER_TOTAL = 4
SSTEP = 4
CG_BLOCKS = 3
GRID_WIDTH_X = 1536
GRID_WIDTH_Y = 512
N_BLK = 16


def set_ends(drawn, own_key, low, largest):
    dims = drawn.shape
    index_at = [jax.random.randint(jax.random.fold_in(own_key, axis), (), 0, dims[axis]) for axis in range(len(dims))]
    drawn = drawn.at[tuple(index_at)].set(low)
    longest = dims.index(max(dims))
    index_at[longest] = (index_at[longest] + 1) % dims[longest]
    return drawn.at[tuple(index_at)].set(largest)


def steps_of(rng, shape, cuts, least, high):
    factor_of, own = 1.0, jax.random.fold_in(rng, 6)
    for axis_at, parts in cuts:
        draws = jnp.exp(jax.random.uniform(jax.random.fold_in(own, axis_at), (parts,), jnp.float32, least / len(cuts), high / len(cuts)))
        factor_of = factor_of * jnp.repeat(draws, shape[axis_at] // parts).reshape([-1 if axis == axis_at else 1 for axis in range(len(shape))])
    return factor_of


def gaussian(own_key, shape, scale, bound, pieces=(), kind=jnp.bfloat16):
    array = jax.random.normal(own_key, shape, jnp.float32) * scale
    if len(pieces) > 0:
        array = steps_of(own_key, shape, pieces, -0.22, 0.18) * array
    return jnp.clip(array, min=-bound, max=bound).astype(kind)


def setup_inputs(seed: int = 0, part: int = 0) -> dict:
    seeds = jax.random.split(jax.random.key(seed), 8)
    part_keys = jax.random.split(jax.random.fold_in(seeds[7], part), 8)
    return {
        "heat_anomaly": gaussian(part_keys[0], (LAYER_TOTAL, GRID_WIDTH_X, GRID_WIDTH_Y), 1.0, 6.0, ((1, 16),), jnp.float32),
        "saltiness_anomaly": gaussian(part_keys[1], (LAYER_TOTAL, GRID_WIDTH_X, GRID_WIDTH_Y), 1.0, 6.0, ((1, 16),), jnp.float32),
        "first_axis_flow": gaussian(part_keys[2], (LAYER_TOTAL, GRID_WIDTH_X, GRID_WIDTH_Y), 1.0, 4.0, ((1, 16),), jnp.float32),
        "second_axis_flow": gaussian(part_keys[3], (LAYER_TOTAL, GRID_WIDTH_X, GRID_WIDTH_Y), 1.0, 4.0, ((1, 16),), jnp.float32),
        "layer_spacing": jnp.clip(jnp.exp(jax.random.uniform(seeds[4], (LAYER_TOTAL,), jnp.float32, math.log(0.5), math.log(4.0))), 0.5, 4.0),
        "diagonal_shift": jnp.clip(jnp.exp(math.log(0.2) - 2.3025851 * jax.random.uniform(seeds[5], (GRID_WIDTH_X, GRID_WIDTH_Y), jnp.float32) ** steps_of(seeds[5], (GRID_WIDTH_X, GRID_WIDTH_Y), ((0, 16),), -0.2, 0.2)), 0.02, 0.2),
        "water_tile_flags": set_ends((jax.random.randint(seeds[6], (N_BLK, HOME), 0, 4) < 3).astype(jnp.int32), jax.random.fold_in(seeds[6], 1), 0, 1),
    }


COURANT = 0.2
HIGHEST = lax.Precision.HIGHEST


def wrap_east(field, margin):
    extent = field.shape[0]
    return jnp.concatenate([field[extent - margin:], field, field[:margin]], axis=0)


def pad_north(field):
    return jnp.pad(field, [(0, 0)] * (field.ndim - 1) + [(1, 1)])


def upwind(speed, behind, ahead):
    return jnp.where(speed > 0.0, speed * behind, speed * ahead)


def advect(tracer, east_vel, north_vel, wet_pad):
    east_face = 0.5 * (east_vel[..., :-1, 1:-1] + east_vel[..., 1:, 1:-1]) * (wet_pad[:-1, 1:-1] * wet_pad[1:, 1:-1])
    east_flux = upwind(east_face, tracer[..., :-1, 1:-1], tracer[..., 1:, 1:-1])
    north_face = 0.5 * (north_vel[..., 1:-1, :-1] + north_vel[..., 1:-1, 1:]) * (wet_pad[1:-1, :-1] * wet_pad[1:-1, 1:])
    north_flux = upwind(north_face, tracer[..., 1:-1, :-1], tracer[..., 1:-1, 1:])
    spread = (east_flux[..., 1:, :] - east_flux[..., :-1, :]) + (north_flux[..., 1:] - north_flux[..., :-1])
    return wet_pad[1:-1, 1:-1] * (tracer[..., 1:-1, 1:-1] - COURANT * spread)


def operate(field_band, wet_band, damp_core):
    values = pad_north(field_band)
    wetness = pad_north(wet_band)
    masked = wetness * values
    edges = (masked[:-2, 1:-1] + masked[2:, 1:-1]) + (masked[1:-1, :-2] + masked[1:-1, 2:])
    corners = (masked[:-2, :-2] + masked[:-2, 2:]) + (masked[2:, :-2] + masked[2:, 2:])
    centre = values[1:-1, 1:-1]
    wet_core = wetness[1:-1, 1:-1]
    return 0.125 * (wet_core * ((6.0 + damp_core) * centre - (edges + 0.5 * corners)) + (1.0 - wet_core) * centre)


def chebyshev_next(image, current, previous):
    if previous is None:
        return 2.0 * image - current
    return 4.0 * image - 2.0 * current - previous


def shift_table(powers):
    extent = 2 * powers + 1
    table = np.zeros((extent, extent), np.float32)
    for offset, count in ((0, powers), (powers + 1, powers - 1)):
        for place in range(count):
            source = offset + place
            if place == 0:
                table[source + 1, source] = 0.5
                table[source, source] = 0.5
            else:
                table[source + 1, source] = 0.25
                table[source, source] = 0.5
                table[source - 1, source] = 0.25
    return table


def inner_steps(gram, powers):
    extent = 2 * powers + 1
    table = jnp.asarray(shift_table(powers), gram.dtype)
    unit = jnp.eye(extent, dtype=gram.dtype)
    along = unit[0]
    resid = unit[powers + 1]
    offset = jnp.zeros((extent,), gram.dtype)
    for sweep in range(powers):
        norm_now = jnp.dot(resid, jnp.dot(gram, resid, precision=HIGHEST), precision=HIGHEST)
        image = jnp.dot(table, along, precision=HIGHEST)
        alpha = norm_now / jnp.dot(along, jnp.dot(gram, image, precision=HIGHEST), precision=HIGHEST)
        offset = offset + alpha * along
        resid = resid - alpha * image
        norm_next = jnp.dot(resid, jnp.dot(gram, resid, precision=HIGHEST), precision=HIGHEST)
        along = resid + (norm_next / norm_now) * along
    return offset, resid, along


def reference(heat_anomaly, saltiness_anomaly, first_axis_flow, second_axis_flow, layer_spacing, diagonal_shift, water_tile_flags):
    ocean = jnp.repeat(jnp.repeat(water_tile_flags.astype(diagonal_shift.dtype), BX, axis=0), BY, axis=1)
    wet_band = wrap_east(ocean, 1)
    wet_pad = pad_north(wet_band)

    def column_layer_advance(layers):
        padded = [pad_north(wrap_east(layer, 1)) for layer in layers]
        return jnp.stack([advect(tracer, padded[2], padded[3], wet_pad) for tracer in padded])

    stepped_fields = lax.map(column_layer_advance, (heat_anomaly, saltiness_anomaly, first_axis_flow, second_axis_flow))
    weights = layer_spacing / jnp.sum(layer_spacing)
    transport_u = jnp.einsum("k,kxy->xy", weights, stepped_fields[:, 2], precision=HIGHEST)
    transport_v = jnp.einsum("k,kxy->xy", weights, stepped_fields[:, 3], precision=HIGHEST)
    east_band = wrap_east(transport_u, 1)
    north_pad = pad_north(transport_v)
    forcing = ocean * (0.5 * ((east_band[2:] - east_band[:-2]) + (north_pad[:, 2:] - north_pad[:, :-2])))

    def apply_whole(field):
        return operate(wrap_east(field, 1), wet_band, diagonal_shift)

    def chebyshev_list(start, count):
        result = [start]
        previous = None
        for power in range(count):
            following = chebyshev_next(apply_whole(result[-1]), result[-1], previous)
            previous = result[-1]
            result.append(following)
        return result

    height = jnp.zeros_like(forcing)
    resid = forcing
    along = forcing
    for outer in range(CG_BLOCKS):
        along_list = chebyshev_list(along, SSTEP)
        resid_list = chebyshev_list(resid, SSTEP - 1)
        basis = jnp.stack(along_list + resid_list)
        gram = jnp.einsum("aij,bij->ab", basis, basis, precision=HIGHEST)
        offset, resid_coef, along_coef = inner_steps(gram, SSTEP)
        height = height + jnp.einsum("a,aij->ij", offset, basis, precision=HIGHEST)
        resid = jnp.einsum("a,aij->ij", resid_coef, basis, precision=HIGHEST)
        along = jnp.einsum("a,aij->ij", along_coef, basis, precision=HIGHEST)
    return (stepped_fields[:, 0].astype(jnp.bfloat16), stepped_fields[:, 1].astype(jnp.bfloat16),
            stepped_fields[:, 2].astype(jnp.bfloat16), stepped_fields[:, 3].astype(jnp.bfloat16), height, resid)
```

```python
import functools

import jax
import jax.numpy as jnp
import numpy as np
from jax import lax
from jax.experimental import pallas as pl
from jax.experimental.pallas import tpu as pltpu
from jax.sharding import PartitionSpec as P

SSTEP = 4
CG_BLOCKS = 3
COURANT = 0.2
DEEP = 16
PAD = 8
STRIP = 16
NEAR = 8
F32 = jnp.float32
HIGHEST = lax.Precision.HIGHEST


def shift_table(powers):
    extent = 2 * powers + 1
    table = np.zeros((extent, extent), np.float32)
    for offset, count in ((0, powers), (powers + 1, powers - 1)):
        for place in range(count):
            source = offset + place
            if place == 0:
                table[source + 1, source] = 0.5
                table[source, source] = 0.5
            else:
                table[source + 1, source] = 0.25
                table[source, source] = 0.5
                table[source - 1, source] = 0.25
    return table


def quadratic(gram, left, right):
    total = None
    for i, li in enumerate(left):
        if li is None:
            continue
        row = None
        for j, rj in enumerate(right):
            if rj is None:
                continue
            term = gram[i][j] * rj
            row = term if row is None else row + term
        term = li * row
        total = term if total is None else total + term
    return total


def plus(a, b):
    if a is None:
        return b
    if b is None:
        return a
    return a + b


def scaled(scale, a):
    return None if a is None else scale * a


def inner_steps(gram, powers):
    extent = 2 * powers + 1
    table = shift_table(powers)
    one = jnp.ones_like(gram[0][0])
    along = [one if i == 0 else None for i in range(extent)]
    resid = [one if i == powers + 1 else None for i in range(extent)]
    offset = [None] * extent
    norm_now = quadratic(gram, resid, resid)
    for sweep in range(powers):
        image = []
        for i in range(extent):
            total = None
            for j in range(extent):
                if table[i, j] != 0.0:
                    total = plus(total, scaled(float(table[i, j]), along[j]))
            image.append(total)
        alpha = norm_now / quadratic(gram, along, image)
        offset = [plus(o, scaled(alpha, a)) for o, a in zip(offset, along)]
        resid = [plus(r, scaled(-alpha, a)) for r, a in zip(resid, image)]
        norm_next = quadratic(gram, resid, resid)
        beta = norm_next / norm_now
        along = [plus(r, scaled(beta, a)) for r, a in zip(resid, along)]
        norm_now = norm_next
    return offset, resid, along


def kernel(
    n,
    heat, salt, uvel, vvel, spacing, damp, flags,
    o_heat, o_salt, o_u, o_v, o_height, o_resid,
    ue, ve, he, se, de, oc, oce, a4, tu, tv, basis, hgt, res,
    bh, bs, bu, bv, pairs, slots,
    lsem, osem, hs_sem, hr_sem, gs_sem, gr_sem,
):
    levels, rows, lanes = uvel.shape
    base = PAD + DEEP
    total = rows + 2 * base
    me = lax.axis_index("blk")
    right, left = lax.rem(me + 1, n), lax.rem(me + n - 1, n)

    loads = [
        pltpu.make_async_copy(uvel, ue.at[:, pl.ds(base, rows)], lsem.at[0]),
        pltpu.make_async_copy(vvel, ve.at[:, pl.ds(base, rows)], lsem.at[1]),
        pltpu.make_async_copy(damp, de.at[pl.ds(base, rows)], lsem.at[2]),
        pltpu.make_async_copy(heat, he.at[:, pl.ds(NEAR, rows)], lsem.at[3]),
        pltpu.make_async_copy(salt, se.at[:, pl.ds(NEAR, rows)], lsem.at[4]),
    ]
    for load in loads:
        load.start()

    barrier = pltpu.get_barrier_semaphore()
    for k in range(1, n):
        pl.semaphore_signal(
            barrier, inc=1, device_id={"blk": lax.rem(me + k, n)},
            device_id_type=pl.DeviceIdType.MESH,
        )

    tiles = flags.shape[1]
    lane_tile = lax.broadcasted_iota(jnp.int32, (8, lanes), 1) // (lanes // tiles)
    own = jnp.zeros((8, lanes), F32)
    for k in range(tiles):
        own = jnp.where(lane_tile == k, flags[0, k].astype(F32), own)
    oc[1] = own
    for ref in (ue, ve):
        ref[:, 0:PAD] = jnp.zeros((levels, PAD, lanes), F32)
        ref[:, total - PAD : total] = jnp.zeros((levels, PAD, lanes), F32)
    for ref in (oce, tu):
        ref[0:PAD] = jnp.zeros((PAD, lanes), F32)
        ref[total - PAD : total] = jnp.zeros((PAD, lanes), F32)
    for k in range(2 * SSTEP + 1):
        basis[k, 0 : 2 * PAD] = jnp.zeros((2 * PAD, lanes), F32)
        basis[k, total - 2 * PAD : total] = jnp.zeros((2 * PAD, lanes), F32)
    pairs[...] = jnp.zeros_like(pairs)
    for r in range(base, base + rows, 8):
        oce[r : r + 8] = own

    pl.semaphore_wait(barrier, n - 1)

    sends = []

    def send(k, src, dst, to, way):
        copy = pltpu.make_async_remote_copy(
            src_ref=src, dst_ref=dst,
            send_sem=hs_sem.at[k, way], recv_sem=hr_sem.at[k, way],
            device_id={"blk": to}, device_id_type=pl.DeviceIdType.MESH,
        )
        copy.start()
        sends.append(copy)
        return copy

    halos = {}

    def exchange3(k, ref, start, depth):
        halos[k] = [
            send(k, ref.at[:, pl.ds(start + rows - depth, depth)],
                 ref.at[:, pl.ds(start - depth, depth)], right, 0),
            send(k, ref.at[:, pl.ds(start, depth)],
                 ref.at[:, pl.ds(start + rows, depth)], left, 1),
        ]

    halos[3] = [
        send(3, oc.at[1], oc.at[0], right, 0),
        send(3, oc.at[1], oc.at[2], left, 1),
    ]
    loads[0].wait()
    exchange3(0, ue, base, DEEP)
    loads[1].wait()
    exchange3(1, ve, base, DEEP)
    loads[2].wait()
    halos[2] = [
        send(2, de.at[pl.ds(base + rows - DEEP, DEEP)],
             de.at[pl.ds(base - DEEP, DEEP)], right, 0),
        send(2, de.at[pl.ds(base, DEEP)],
             de.at[pl.ds(base + rows, DEEP)], left, 1),
    ]
    loads[3].wait()
    exchange3(4, he, NEAR, NEAR)
    loads[4].wait()
    exchange3(5, se, NEAR, NEAR)

    lane = lax.broadcasted_iota(jnp.int32, (STRIP, lanes), 1)

    def north_of(x):
        return pltpu.roll(x, lanes - 1, 1)

    def south_of(x):
        return pltpu.roll(x, 1, 1)

    def faces(level, r):
        here = pl.ds(r, STRIP)
        u0, up, um = ue[level, here], ue[level, pl.ds(r + 1, STRIP)], ue[level, pl.ds(r - 1, STRIP)]
        v0 = ve[level, here]
        w0, wp, wm = oce[here], oce[pl.ds(r + 1, STRIP)], oce[pl.ds(r - 1, STRIP)]
        east = 0.5 * (u0 + up) * (w0 * wp)
        west = 0.5 * (um + u0) * (wm * w0)
        ahead = jnp.where(lane == lanes - 1, 0.0, w0 * north_of(w0))
        north = 0.5 * (v0 + north_of(v0)) * ahead
        return east, west, north, w0

    def advect(face, ref, level, r):
        east, west, north, w0 = face
        q0, qp, qm = ref[level, pl.ds(r, STRIP)], ref[level, pl.ds(r + 1, STRIP)], ref[level, pl.ds(r - 1, STRIP)]
        fe = east * jnp.where(east > 0.0, q0, qp)
        fw = west * jnp.where(west > 0.0, qm, q0)
        fn = north * jnp.where(north > 0.0, q0, north_of(q0))
        return w0 * (q0 - COURANT * ((fe - fw) + (fn - south_of(fn))))

    strips = list(range(PAD, total - PAD, STRIP))
    inner = [r for r in strips if r >= base + STRIP and r + STRIP < base + rows]
    outer = [r for r in strips if r not in inner]

    whole_w = jnp.zeros((8, 128), F32)
    for j in range(levels):
        whole_w = whole_w + spacing[j]
    portions = [(jnp.full((8, 128), spacing[j], F32) / whole_w)[0:1, 0:1] for j in range(levels)]

    def flows(which):
        for level in range(levels):
            for r in which:
                face = faces(level, r)
                for ref, acc, out in ((ue, tu, bu), (ve, tv, bv)):
                    new = advect(face, ref, level, r)
                    part = portions[level] * new
                    here = pl.ds(r, STRIP)
                    acc[here] = part if level == 0 else acc[here] + part
                    if base <= r < base + rows:
                        out[level, r - base : r - base + STRIP] = new.astype(jnp.bfloat16)

    flows(inner)

    for k in (3, 0, 1):
        for copy in halos[k]:
            copy.wait_recv()
    for r in range(PAD, base, 8):
        oce[r : r + 8] = oc[0]
    for r in range(base + rows, total - PAD, 8):
        oce[r : r + 8] = oc[2]

    flows(outer)
    stores = [
        pltpu.make_async_copy(bu, o_u, osem.at[0]),
        pltpu.make_async_copy(bv, o_v, osem.at[1]),
    ]
    for store in stores:
        store.start()

    for copy in halos[2]:
        copy.wait_recv()
    for r in strips:
        here = pl.ds(r, STRIP)
        w0 = oce[here]
        a4[here] = 0.5 * (w0 * (6.0 + de[here]) + (1.0 - w0)) - 2.0
        t0 = tv[here]
        north = jnp.where(lane == lanes - 1, 0.0, north_of(t0))
        south = jnp.where(lane == 0, 0.0, south_of(t0))
        east = tu[pl.ds(r + 1, STRIP)] - tu[pl.ds(r - 1, STRIP)]
        basis[0, here] = w0 * (0.5 * (east + (north - south)))

    def pieces(first, last):
        cuts, r = [], first
        while r < last:
            h = STRIP if r % STRIP == PAD % STRIP and r + STRIP <= last else 8
            cuts.append((r, h))
            r += h
        return cuts

    def chebyshev(cur, nxt, prev, first, last):
        for r, h in pieces(first, last):
            here = pl.ds(r, h)
            k0 = basis[cur, here]
            ku, kd = basis[cur, pl.ds(r - 1, h)], basis[cur, pl.ds(r + 1, h)]
            w0 = oce[here]
            if r in (base, base + rows) or r + h in (base, base + rows):
                ku = ku * oce[pl.ds(r - 1, h)]
                kd = kd * oce[pl.ds(r + 1, h)]
                vert = ku + kd
                z = w0 * k0 + 0.5 * vert
            else:
                vert = ku + kd
                z = w0 * (k0 + 0.5 * vert)
            ln = lane[0:h]
            side = jnp.where(ln == 0, 0.0, south_of(z)) + jnp.where(ln == lanes - 1, 0.0, north_of(z))
            half = a4[here] * k0 - (0.5 * w0) * (vert + side)
            basis[nxt, here] = 0.5 * half if prev is None else half - basis[prev, here]

    def gram_partial(count):
        pair_list = [(a, b) for a in range(count) for b in range(a, count)]

        def body(s, accs):
            r = pl.multiple_of(base + 8 * s, 8)
            accs = list(accs)
            for c in range(0, lanes, 128):
                vals = [basis[a, pl.ds(r, 8), c : c + 128] for a in range(count)]
                for i, (a, b) in enumerate(pair_list):
                    accs[i] = accs[i] + vals[a] * vals[b]
            return tuple(accs)

        accs = lax.fori_loop(
            0, rows // 8, body, tuple(jnp.zeros((8, 128), F32) for _ in pair_list)
        )
        for i, acc in enumerate(accs):
            pairs[i : i + 1, :] = jnp.sum(acc, axis=0, keepdims=True)
        ones = jnp.ones((8, 128), F32)
        sums = lax.dot_general(
            ones, pairs[...], (((1,), (1,)), ((), ())),
            precision=HIGHEST, preferred_element_type=F32,
        )
        return pair_list, sums[0:1]

    def gram_send(b, row):
        slots[b, me] = row
        copies = []
        for k in range(1, n):
            to = lax.rem(me + k, n)
            copy = pltpu.make_async_remote_copy(
                src_ref=slots.at[b, me], dst_ref=slots.at[b, me],
                send_sem=gs_sem.at[b, k], recv_sem=gr_sem.at[b, k],
                device_id={"blk": to}, device_id_type=pl.DeviceIdType.MESH,
            )
            copy.start()
            copies.append(copy)
        return copies

    def gram_take(b, copies, pair_list):
        for k in range(1, n):
            src = lax.rem(me + n - k, n)
            pltpu.make_async_remote_copy(
                src_ref=slots.at[b, src], dst_ref=slots.at[b, src],
                send_sem=gs_sem.at[b, k], recv_sem=gr_sem.at[b, k],
                device_id={"blk": src}, device_id_type=pl.DeviceIdType.MESH,
            ).wait_recv()
        row = slots[b, 0]
        for i in range(1, n):
            row = row + slots[b, i]
        row = jnp.broadcast_to(row, (8, 128))
        return {
            pair: jnp.broadcast_to(row[:, i : i + 1], (8, 128))
            for i, pair in enumerate(pair_list)
        }

    def tracers(chosen):
        for level in chosen:
            for r in range(0, rows, STRIP):
                face = faces(level, base + r)
                here = pl.ds(r, STRIP)
                bh[level, here] = advect(face, he, level, NEAR + r).astype(jnp.bfloat16)
                bs[level, here] = advect(face, se, level, NEAR + r).astype(jnp.bfloat16)

    shares = [list(range(levels))[i::CG_BLOCKS] for i in range(CG_BLOCKS)]
    group = SSTEP + 1
    for b in range(CG_BLOCKS):
        depth = DEEP if b == 0 else 8
        first, last = base - depth, base + rows + depth
        for p in range(SSTEP):
            chebyshev(p, p + 1, None if p == 0 else p - 1, first, last)
        if b > 0:
            for p in range(SSTEP - 1):
                q = group + p
                chebyshev(q, q + 1, None if p == 0 else q - 1, first, last)
        count = group if b == 0 else 2 * SSTEP + 1
        pair_list, row = gram_partial(count)
        copies = gram_send(b, row)
        if b == 0:
            for k in (4, 5):
                for copy in halos[k]:
                    copy.wait_recv()
        tracers(shares[b])
        if b == CG_BLOCKS - 1:
            for k, (buf, out) in enumerate(((bh, o_heat), (bs, o_salt))):
                store = pltpu.make_async_copy(buf, out, osem.at[2 + k])
                store.start()
                stores.append(store)
        got = gram_take(b, copies, pair_list)

        def place(i):
            return i - group if b == 0 and i >= group else i

        gram = [
            [got[tuple(sorted((place(i), place(j))))] for j in range(2 * SSTEP + 1)]
            for i in range(2 * SSTEP + 1)
        ]
        coefs = inner_steps(gram, SSTEP)
        merged = []
        for coef in coefs:
            out = [None] * count
            for i, c in enumerate(coef):
                out[place(i)] = plus(out[place(i)], c)
            merged.append(out)
        offset, resid, along = merged
        final = b == CG_BLOCKS - 1

        def combine(vals, coef):
            out = None
            for v, c in zip(vals, coef):
                if c is not None:
                    out = plus(out, c * v)
            return out

        def update(s, carry, own_rows):
            r = pl.multiple_of(s * 8, 8)
            for c in range(0, lanes, 128):
                here = (pl.ds(r, 8), slice(c, c + 128))
                vals = [basis[(i,) + here] for i in range(count)]
                if own_rows:
                    to = (pl.ds(pl.multiple_of(r - base, 8), 8), slice(c, c + 128))
                    step = combine(vals, offset)
                    hgt[to] = step if b == 0 else hgt[to] + step
                if final:
                    res[to] = combine(vals, resid)
                else:
                    basis[(group,) + here] = combine(vals, resid)
                    basis[(0,) + here] = combine(vals, along)
            return carry

        if not final:
            for r in (base - 8, base + rows):
                update(r // 8, 0, False)
        lax.fori_loop(base // 8, (base + rows) // 8, lambda s, c: update(s, c, True), 0)
        for copy in copies:
            copy.wait_send()

    for k, (buf, out) in enumerate(((hgt, o_height), (res, o_resid))):
        store = pltpu.make_async_copy(buf, out, osem.at[4 + k])
        store.start()
        stores.append(store)
    for copy in sends:
        copy.wait_send()
    for store in stores:
        store.wait()


def on_device(heat, salt, uvel, vvel, spacing, damp, flags):
    n = lax.axis_size("blk")
    levels, rows, lanes = uvel.shape
    total = rows + 2 * (PAD + DEEP)
    near = rows + 2 * NEAR
    hbm = pl.BlockSpec(memory_space=pl.ANY)
    smem = pl.BlockSpec(memory_space=pltpu.SMEM)
    half = jax.ShapeDtypeStruct((levels, rows, lanes), jnp.bfloat16)
    flat = jax.ShapeDtypeStruct((rows, lanes), F32)
    vm = pltpu.VMEM
    return pl.pallas_call(
        functools.partial(kernel, n),
        out_shape=(half, half, half, half, flat, flat),
        in_specs=[hbm, hbm, hbm, hbm, smem, hbm, smem],
        out_specs=(hbm,) * 6,
        scratch_shapes=[
            vm((levels, total, lanes), F32),
            vm((levels, total, lanes), F32),
            vm((levels, near, lanes), F32),
            vm((levels, near, lanes), F32),
            vm((total, lanes), F32),
            vm((3, 8, lanes), F32),
            vm((total, lanes), F32),
            vm((total, lanes), F32),
            vm((total, lanes), F32),
            vm((total, lanes), F32),
            vm((2 * SSTEP + 1, total, lanes), F32),
            vm((rows, lanes), F32),
            vm((rows, lanes), F32),
            vm((levels, rows, lanes), jnp.bfloat16),
            vm((levels, rows, lanes), jnp.bfloat16),
            vm((levels, rows, lanes), jnp.bfloat16),
            vm((levels, rows, lanes), jnp.bfloat16),
            vm((128, 128), F32),
            vm((CG_BLOCKS, n, 1, 128), F32),
            pltpu.SemaphoreType.DMA((5,)),
            pltpu.SemaphoreType.DMA((6,)),
            pltpu.SemaphoreType.DMA((6, 2)),
            pltpu.SemaphoreType.DMA((6, 2)),
            pltpu.SemaphoreType.DMA((CG_BLOCKS, n)),
            pltpu.SemaphoreType.DMA((CG_BLOCKS, n)),
        ],
        compiler_params=pltpu.CompilerParams(
            collective_id=0, has_side_effects=True, vmem_limit_bytes=48 * 1024 * 1024
        ),
    )(heat, salt, uvel, vvel, spacing, damp, flags)


def solution(mesh):
    return jax.shard_map(
        on_device,
        mesh=mesh,
        in_specs=(
            P("member", "blk", None),
            P("member", "blk", None),
            P("member", "blk", None),
            P("member", "blk", None),
            P(),
            P("blk", None),
            P("blk", None),
        ),
        out_specs=(
            P("member", "blk", None),
            P("member", "blk", None),
            P("member", "blk", None),
            P("member", "blk", None),
            P(("member", "blk"), None),
            P(("member", "blk"), None),
        ),
        check_vma=False,
    )
```

```python
import functools

import jax
import jax.numpy as jnp
import numpy as np
from jax import lax
from jax.experimental import pallas as pl
from jax.experimental.pallas import tpu as pltpu
from jax.sharding import PartitionSpec as P

SSTEP = 4
CG_BLOCKS = 3
SWEEPS = SSTEP * CG_BLOCKS
FIELDS = SWEEPS + 1
COURANT = 0.2
DEEP = 16
PAD = 8
STRIP = 16
NEAR = 8
F32 = jnp.float32
HIGHEST = lax.Precision.HIGHEST


def shift_table(extent):
    table = np.zeros((extent, extent), np.float32)
    for source in range(extent - 1):
        if source == 0:
            table[1, 0] = table[0, 0] = 0.5
        else:
            table[source + 1, source] = 0.25
            table[source, source] = 0.5
            table[source - 1, source] = 0.25
    return table


def tree(terms):
    while len(terms) > 1:
        terms = [
            terms[i] + terms[i + 1] if i + 1 < len(terms) else terms[i]
            for i in range(0, len(terms), 2)
        ]
    return terms[0]


def quadratic(gram, left, right):
    rows = []
    for i, li in enumerate(left):
        if li is not None:
            rows.append(li * tree([gram[i][j] * rj for j, rj in enumerate(right) if rj is not None]))
    return tree(rows)


def plus(a, b):
    if a is None:
        return b
    if b is None:
        return a
    return a + b


def scaled(scale, a):
    return None if a is None else scale * a


def inner_steps(gram, sweeps):
    extent = sweeps + 1
    table = shift_table(extent)
    one = jnp.ones_like(gram[0][0])
    along = [one] + [None] * sweeps
    resid = [one] + [None] * sweeps
    offset = [None] * extent
    norm_now = quadratic(gram, resid, resid)
    for sweep in range(sweeps):
        image = []
        for i in range(extent):
            total = None
            for j in range(extent):
                if table[i, j] != 0.0:
                    total = plus(total, scaled(float(table[i, j]), along[j]))
            image.append(total)
        alpha = norm_now / quadratic(gram, along, image)
        offset = [plus(o, scaled(alpha, a)) for o, a in zip(offset, along)]
        resid = [plus(r, scaled(-alpha, a)) for r, a in zip(resid, image)]
        if sweep + 1 < sweeps:
            norm_next = quadratic(gram, resid, resid)
            beta = norm_next / norm_now
            along = [plus(r, scaled(beta, a)) for r, a in zip(resid, along)]
            norm_now = norm_next
    return offset, resid


def kernel(
    n,
    heat, salt, uvel, vvel, spacing, damp, flags,
    o_heat, o_salt, o_u, o_v, o_height, o_resid,
    ue, ve, he, se, de, oc, oce, a4, tu, tv, basis, hgt, res,
    bh, bs, bu, bv, pairs, slots,
    lsem, osem, hs_sem, hr_sem, gs_sem, gr_sem,
):
    levels, rows, lanes = uvel.shape
    base = PAD + DEEP
    total = rows + 2 * base
    me = lax.axis_index("blk")
    right, left = lax.rem(me + 1, n), lax.rem(me + n - 1, n)

    loads = [
        pltpu.make_async_copy(uvel, ue.at[:, pl.ds(base, rows)], lsem.at[0]),
        pltpu.make_async_copy(vvel, ve.at[:, pl.ds(base, rows)], lsem.at[1]),
        pltpu.make_async_copy(damp, de.at[pl.ds(base, rows)], lsem.at[2]),
        pltpu.make_async_copy(heat, he.at[:, pl.ds(NEAR, rows)], lsem.at[3]),
        pltpu.make_async_copy(salt, se.at[:, pl.ds(NEAR, rows)], lsem.at[4]),
    ]
    for load in loads:
        load.start()

    barrier = pltpu.get_barrier_semaphore()
    for k in range(1, n):
        pl.semaphore_signal(
            barrier, inc=1, device_id={"blk": lax.rem(me + k, n)},
            device_id_type=pl.DeviceIdType.MESH,
        )

    tiles = flags.shape[1]
    lane_tile = lax.broadcasted_iota(jnp.int32, (8, lanes), 1) // (lanes // tiles)
    own = jnp.zeros((8, lanes), F32)
    for k in range(tiles):
        own = jnp.where(lane_tile == k, flags[0, k].astype(F32), own)
    oc[1] = own
    for ref in (ue, ve):
        ref[:, 0:PAD] = jnp.zeros((levels, PAD, lanes), F32)
        ref[:, total - PAD : total] = jnp.zeros((levels, PAD, lanes), F32)
    for ref in (oce, tu):
        ref[0:PAD] = jnp.zeros((PAD, lanes), F32)
        ref[total - PAD : total] = jnp.zeros((PAD, lanes), F32)
    for k in range(FIELDS):
        basis[k, 0 : 2 * PAD] = jnp.zeros((2 * PAD, lanes), F32)
        basis[k, total - 2 * PAD : total] = jnp.zeros((2 * PAD, lanes), F32)
    pairs[...] = jnp.zeros_like(pairs)
    for r in range(base, base + rows, 8):
        oce[r : r + 8] = own

    pl.semaphore_wait(barrier, n - 1)

    sends = []

    def send(k, src, dst, to, way):
        copy = pltpu.make_async_remote_copy(
            src_ref=src, dst_ref=dst,
            send_sem=hs_sem.at[k, way], recv_sem=hr_sem.at[k, way],
            device_id={"blk": to}, device_id_type=pl.DeviceIdType.MESH,
        )
        copy.start()
        sends.append(copy)
        return copy

    halos = {}

    def exchange3(k, ref, start, depth):
        halos[k] = [
            send(k, ref.at[:, pl.ds(start + rows - depth, depth)],
                 ref.at[:, pl.ds(start - depth, depth)], right, 0),
            send(k, ref.at[:, pl.ds(start, depth)],
                 ref.at[:, pl.ds(start + rows, depth)], left, 1),
        ]

    halos[3] = [
        send(3, oc.at[1], oc.at[0], right, 0),
        send(3, oc.at[1], oc.at[2], left, 1),
    ]
    loads[0].wait()
    exchange3(0, ue, base, DEEP)
    loads[1].wait()
    exchange3(1, ve, base, DEEP)
    loads[2].wait()
    halos[2] = [
        send(2, de.at[pl.ds(base + rows - DEEP, DEEP)],
             de.at[pl.ds(base - DEEP, DEEP)], right, 0),
        send(2, de.at[pl.ds(base, DEEP)],
             de.at[pl.ds(base + rows, DEEP)], left, 1),
    ]
    loads[3].wait()
    exchange3(4, he, NEAR, NEAR)
    loads[4].wait()
    exchange3(5, se, NEAR, NEAR)

    lane = lax.broadcasted_iota(jnp.int32, (STRIP, lanes), 1)

    def north_of(x):
        return pltpu.roll(x, lanes - 1, 1)

    def south_of(x):
        return pltpu.roll(x, 1, 1)

    def faces(level, r):
        here = pl.ds(r, STRIP)
        u0, up, um = ue[level, here], ue[level, pl.ds(r + 1, STRIP)], ue[level, pl.ds(r - 1, STRIP)]
        v0 = ve[level, here]
        w0, wp, wm = oce[here], oce[pl.ds(r + 1, STRIP)], oce[pl.ds(r - 1, STRIP)]
        east = 0.5 * (u0 + up) * (w0 * wp)
        west = 0.5 * (um + u0) * (wm * w0)
        ahead = jnp.where(lane == lanes - 1, 0.0, w0 * north_of(w0))
        north = 0.5 * (v0 + north_of(v0)) * ahead
        return east, west, north, w0

    def advect(face, ref, level, r):
        east, west, north, w0 = face
        q0, qp, qm = ref[level, pl.ds(r, STRIP)], ref[level, pl.ds(r + 1, STRIP)], ref[level, pl.ds(r - 1, STRIP)]
        fe = east * jnp.where(east > 0.0, q0, qp)
        fw = west * jnp.where(west > 0.0, qm, q0)
        fn = north * jnp.where(north > 0.0, q0, north_of(q0))
        return w0 * (q0 - COURANT * ((fe - fw) + (fn - south_of(fn))))

    strips = list(range(PAD, total - PAD, STRIP))
    inner = [r for r in strips if r >= base + STRIP and r + STRIP < base + rows]
    outer = [r for r in strips if r not in inner]

    whole_w = jnp.zeros((8, 128), F32)
    for j in range(levels):
        whole_w = whole_w + spacing[j]
    portions = [(jnp.full((8, 128), spacing[j], F32) / whole_w)[0:1, 0:1] for j in range(levels)]

    def flows(which):
        for level in range(levels):
            for r in which:
                face = faces(level, r)
                for ref, acc, out in ((ue, tu, bu), (ve, tv, bv)):
                    new = advect(face, ref, level, r)
                    part = portions[level] * new
                    here = pl.ds(r, STRIP)
                    acc[here] = part if level == 0 else acc[here] + part
                    if base <= r < base + rows:
                        out[level, r - base : r - base + STRIP] = new.astype(jnp.bfloat16)

    flows(inner)

    for k in (3, 0, 1):
        for copy in halos[k]:
            copy.wait_recv()
    for r in range(PAD, base, 8):
        oce[r : r + 8] = oc[0]
    for r in range(base + rows, total - PAD, 8):
        oce[r : r + 8] = oc[2]

    flows(outer)
    stores = [
        pltpu.make_async_copy(bu, o_u, osem.at[0]),
        pltpu.make_async_copy(bv, o_v, osem.at[1]),
    ]
    for store in stores:
        store.start()

    for copy in halos[2]:
        copy.wait_recv()
    for r in strips:
        here = pl.ds(r, STRIP)
        w0 = oce[here]
        a4[here] = 0.5 * (w0 * (6.0 + de[here]) + (1.0 - w0)) - 2.0
        t0 = tv[here]
        north = jnp.where(lane == lanes - 1, 0.0, north_of(t0))
        south = jnp.where(lane == 0, 0.0, south_of(t0))
        east = tu[pl.ds(r + 1, STRIP)] - tu[pl.ds(r - 1, STRIP)]
        basis[0, here] = w0 * (0.5 * (east + (north - south)))

    def pieces(first, last):
        cuts, r = [], first
        while r < last:
            h = STRIP if r % STRIP == PAD % STRIP and r + STRIP <= last else 8
            cuts.append((r, h))
            r += h
        return cuts

    def chebyshev(cur, nxt, prev, first, last):
        for r, h in pieces(first, last):
            here = pl.ds(r, h)
            k0 = basis[cur, here]
            ku, kd = basis[cur, pl.ds(r - 1, h)], basis[cur, pl.ds(r + 1, h)]
            w0 = oce[here]
            if r in (base, base + rows) or r + h in (base, base + rows):
                ku = ku * oce[pl.ds(r - 1, h)]
                kd = kd * oce[pl.ds(r + 1, h)]
                vert = ku + kd
                z = w0 * k0 + 0.5 * vert
            else:
                vert = ku + kd
                z = w0 * (k0 + 0.5 * vert)
            ln = lane[0:h]
            side = jnp.where(ln == 0, 0.0, south_of(z)) + jnp.where(ln == lanes - 1, 0.0, north_of(z))
            half = a4[here] * k0 - (0.5 * w0) * (vert + side)
            basis[nxt, here] = 0.5 * half if prev is None else half - basis[prev, here]

    pair_list = [(a, b) for a in range(FIELDS) for b in range(a, FIELDS)]

    def gram_partial(first, chosen):
        def body(s, accs):
            r = pl.multiple_of(base + 8 * s, 8)
            accs = list(accs)
            for c in range(0, lanes, 128):
                vals = [basis[a, pl.ds(r, 8), c : c + 128] for a in range(FIELDS)]
                for i, (a, b) in enumerate(chosen):
                    accs[i] = accs[i] + vals[a] * vals[b]
            return tuple(accs)

        accs = lax.fori_loop(
            0, rows // 8, body, tuple(jnp.zeros((8, 128), F32) for _ in chosen)
        )
        for i, acc in enumerate(accs):
            pairs[first + i : first + i + 1, :] = jnp.sum(acc, axis=0, keepdims=True)

    def tracers(chosen):
        for level in chosen:
            for r in range(0, rows, STRIP):
                face = faces(level, base + r)
                here = pl.ds(r, STRIP)
                bh[level, here] = advect(face, he, level, NEAR + r).astype(jnp.bfloat16)
                bs[level, here] = advect(face, se, level, NEAR + r).astype(jnp.bfloat16)

    for p in range(SWEEPS):
        reach = -(-(SWEEPS - p - 1) // 8) * 8
        chebyshev(p, p + 1, None if p == 0 else p - 1, base - reach, base + rows + reach)
    half = (len(pair_list) + 1) // 2
    gram_partial(0, pair_list[:half])
    gram_partial(half, pair_list[half:])
    sums = lax.dot_general(
        jnp.ones((8, 128), F32), pairs[...], (((1,), (1,)), ((), ())),
        precision=HIGHEST, preferred_element_type=F32,
    )
    slots[me] = sums[0:1]
    copies = []
    for k in range(1, n):
        copy = pltpu.make_async_remote_copy(
            src_ref=slots.at[me], dst_ref=slots.at[me],
            send_sem=gs_sem.at[k], recv_sem=gr_sem.at[k],
            device_id={"blk": lax.rem(me + k, n)}, device_id_type=pl.DeviceIdType.MESH,
        )
        copy.start()
        copies.append(copy)

    for k in (4, 5):
        for copy in halos[k]:
            copy.wait_recv()
    tracers(range(levels))
    for k, (buf, out) in enumerate(((bh, o_heat), (bs, o_salt))):
        store = pltpu.make_async_copy(buf, out, osem.at[2 + k])
        store.start()
        stores.append(store)

    for k in range(1, n):
        src = lax.rem(me + n - k, n)
        pltpu.make_async_remote_copy(
            src_ref=slots.at[src], dst_ref=slots.at[src],
            send_sem=gs_sem.at[k], recv_sem=gr_sem.at[k],
            device_id={"blk": src}, device_id_type=pl.DeviceIdType.MESH,
        ).wait_recv()
    row = jnp.broadcast_to(tree([slots[i] for i in range(n)]), (8, 128))
    gram = [[None] * FIELDS for _ in range(FIELDS)]
    for i, (a, b) in enumerate(pair_list):
        gram[a][b] = gram[b][a] = jnp.broadcast_to(row[:, i : i + 1], (8, 128))
    offset, resid = inner_steps(gram, SWEEPS)

    def combine(vals, coef):
        return tree([c * v for v, c in zip(vals, coef) if c is not None])

    def update(s, carry):
        r = pl.multiple_of(s * 8, 8)
        for c in range(0, lanes, 128):
            vals = [basis[i, pl.ds(pl.multiple_of(base + r, 8), 8), c : c + 128] for i in range(FIELDS)]
            hgt[pl.ds(r, 8), c : c + 128] = combine(vals, offset)
            res[pl.ds(r, 8), c : c + 128] = combine(vals, resid)
        return carry

    lax.fori_loop(0, rows // 8, update, 0)
    for copy in copies:
        copy.wait_send()

    for k, (buf, out) in enumerate(((hgt, o_height), (res, o_resid))):
        store = pltpu.make_async_copy(buf, out, osem.at[4 + k])
        store.start()
        stores.append(store)
    for copy in sends:
        copy.wait_send()
    for store in stores:
        store.wait()


def drain(*refs):
    count = len(refs) // 2
    sems = refs[-1]
    copies = [
        pltpu.make_async_copy(refs[i], refs[count + i], sems.at[i]) for i in range(count)
    ]
    for copy in copies:
        copy.start()
    for copy in copies:
        copy.wait()


def on_device(heat, salt, uvel, vvel, spacing, damp, flags):
    n = lax.axis_size("blk")
    levels, rows, lanes = uvel.shape
    total = rows + 2 * (PAD + DEEP)
    near = rows + 2 * NEAR
    hbm = pl.BlockSpec(memory_space=pltpu.HBM)
    free = pl.BlockSpec(memory_space=pl.ANY)
    smem = pl.BlockSpec(memory_space=pltpu.SMEM)
    heat, salt, uvel, vvel, damp = (
        pltpu.with_memory_space_constraint(x, pltpu.HBM) for x in (heat, salt, uvel, vvel, damp)
    )
    half = jax.ShapeDtypeStruct((levels, rows, lanes), jnp.bfloat16)
    flat = jax.ShapeDtypeStruct((rows, lanes), F32)
    vm = pltpu.VMEM
    shapes = (half, half, half, half, flat, flat)
    results = pl.pallas_call(
        functools.partial(kernel, n),
        out_shape=shapes,
        in_specs=[hbm, hbm, hbm, hbm, smem, hbm, smem],
        out_specs=(free,) * 6,
        scratch_shapes=[
            vm((levels, total, lanes), F32),
            vm((levels, total, lanes), F32),
            vm((levels, near, lanes), F32),
            vm((levels, near, lanes), F32),
            vm((total, lanes), F32),
            vm((3, 8, lanes), F32),
            vm((total, lanes), F32),
            vm((total, lanes), F32),
            vm((total, lanes), F32),
            vm((total, lanes), F32),
            vm((FIELDS, total, lanes), F32),
            vm((rows, lanes), F32),
            vm((rows, lanes), F32),
            vm((levels, rows, lanes), jnp.bfloat16),
            vm((levels, rows, lanes), jnp.bfloat16),
            vm((levels, rows, lanes), jnp.bfloat16),
            vm((levels, rows, lanes), jnp.bfloat16),
            vm((128, 128), F32),
            vm((n, 1, 128), F32),
            pltpu.SemaphoreType.DMA((5,)),
            pltpu.SemaphoreType.DMA((6,)),
            pltpu.SemaphoreType.DMA((6, 2)),
            pltpu.SemaphoreType.DMA((6, 2)),
            pltpu.SemaphoreType.DMA((n,)),
            pltpu.SemaphoreType.DMA((n,)),
        ],
        compiler_params=pltpu.CompilerParams(
            collective_id=0, has_side_effects=True, vmem_limit_bytes=48 * 1024 * 1024
        ),
    )(heat, salt, uvel, vvel, spacing, damp, flags)
    results = [pltpu.with_memory_space_constraint(x, pltpu.VMEM) for x in results]
    return pl.pallas_call(
        drain,
        out_shape=tuple(pltpu.HBM(x.shape, x.dtype) for x in shapes),
        in_specs=[pl.BlockSpec(memory_space=pltpu.VMEM)] * 6,
        out_specs=(hbm,) * 6,
        scratch_shapes=[pltpu.SemaphoreType.DMA((6,))],
    )(*results)


def solution(mesh):
    return jax.shard_map(
        on_device,
        mesh=mesh,
        in_specs=(
            P("member", "blk", None),
            P("member", "blk", None),
            P("member", "blk", None),
            P("member", "blk", None),
            P(),
            P("blk", None),
            P("blk", None),
        ),
        out_specs=(
            P("member", "blk", None),
            P("member", "blk", None),
            P("member", "blk", None),
            P("member", "blk", None),
            P(("member", "blk"), None),
            P(("member", "blk"), None),
        ),
        check_vma=False,
    )
```
